32 devices in a mesh: grp: 2 (over core), dev: 16 (over z, y, x).
Axes of the slice: x: 2, y: 2, z: 4, core: 2. Of those that a mesh axis runs over, the one named last changes fastest.
Arguments:
- pixel_tiles: float32 [2048, 6, 512], P(('grp', 'dev')), may hold values from -31 to 31
- blend_source: int32 [2048, 2], P(('grp', 'dev')), may hold values from 0 to 15, all different within a row; in each aligned block of 64 rows (0 to 63, 64 to 127, ...) at most 8 rows name the same one
- blend_slot: int32 [2048, 2], P(('grp', 'dev')), may hold values from 0 to 63
- component_count: int32 [2048], P(('grp', 'dev')), may hold values from 12 to 24
- sed_start: bfloat16 [2048, 24, 6], P(('grp', 'dev')), may hold values from 0.049804688 to 0.5
- morph_start: bfloat16 [2048, 2, 24, 512], P(('grp', 'dev')), may hold values from 0.019897461 to 0.5
Outputs:
- whitened: float32 [2048, 6, 512], P(('grp', 'dev'))
- sed_final: bfloat16 [2048, 24, 6], P(('grp', 'dev'))
The draws below stay inside these ranges and needn't reach their ends.
Inputs may be any that keep to these rules, and one draw needn't show every extreme that they name: `blend_source`: each blend names 2 different devices of its region; over the blends of one device no device is named more than 8 times, and some device is named exactly 8 times. `blend_slot`: several blends may name the same tile.
All inputs are finite; a program needn't handle non-finite values.
Results may differ from the reference program's by a relative error of at most 0.0052.
Values may be sent and summed in bfloat16 or wider, within the bound.
No kernel may reach another device: no remote copies, remote signals or barrier semaphores. Data moves between devices by JAX's collectives and lax.ppermute only.
A program may use at most 64 MiB of HBM per device.

```python
import math
import jax
import jax.numpy as jnp
import numpy as np
from jax import lax

BANDS = 6
COMPONENTS = 24
PIX = 512
FOOT = 2
ITERS = 2
TILE_DEV = 64
BLEND_DEV = 64
CAPACITY = 8
TILES_G = 1024
BLENDS_G = 1024
TILES_ALL = 2048
BLENDS_ALL = 2048
N_DEV = 16


def draw_pixel_tiles(key, part):
    key_base, key_rough = jax.random.split(jax.random.fold_in(key, 11), 2)
    shape = (TILES_ALL, BANDS, PIX)
    position = (jnp.arange(TILES_ALL, dtype=jnp.int32) % TILES_G).astype(jnp.float32) / TILES_G
    rough = jnp.exp(jax.random.uniform(key_rough, (TILES_ALL, 1, 1), jnp.float32, -0.7, 0.7))
    scale = jnp.power(3.0, position)[:, None, None] * rough
    base = jnp.clip(jax.random.normal(key_base, shape, jnp.float32), -5.0, 5.0)
    return (base * scale).astype(jnp.float32)


def with_ends(drawn, stream_key, low, top_value):
    index_at = [jax.random.randint(jax.random.fold_in(stream_key, axis), (), 0, length) for axis, length in enumerate(drawn.shape)]
    widest = drawn.shape.index(max(drawn.shape))
    next_to = index_at[:widest] + [(index_at[widest] + 1) % drawn.shape[widest]] + index_at[widest + 1:]
    return drawn.at[tuple(index_at)].set(low).at[tuple(next_to)].set(top_value)


def levels(stream_key, extent, pieces, smallest, high):
    def one(axis_at, parts):
        heights = jax.random.uniform(jax.random.fold_in(jax.random.fold_in(stream_key, 6), axis_at), (parts,), jnp.float32, smallest / len(pieces), high / len(pieces))
        return jnp.repeat(jnp.exp(heights), extent[axis_at] // parts).reshape((-1,) + (1,) * (len(extent) - axis_at - 1))

    factor_of = one(*pieces[0])
    for cut in pieces[1:]:
        factor_of = factor_of * one(*cut)
    return factor_of


def shared_out(rng, own, number, rows, amount, top, most, skew):
    sequence = jax.random.permutation(rng, amount)
    packed, ordinary = load_shares(amount, rows * top, most, skew, True), load_shares(amount, rows * top, most, skew, False)
    places = jnp.arange(amount)

    def named(tallies, turn):
        used = int((tallies > 0).sum())
        fixed = max(1, used // 4)
        shifted = fixed + (places - fixed + turn * (used - fixed)) % max(1, amount - fixed)
        return jnp.zeros((amount,), jnp.int32).at[sequence[jnp.where(places < fixed, places, shifted)]].set(jnp.asarray(tallies, jnp.int32))

    tallies = jnp.where(number % 4 == 0, named(packed, number // 4), named(ordinary, number - number // 4 - 1))
    mixed = jax.random.permutation(jax.random.fold_in(own, 3), amount)
    donor, taker = mixed[0:amount // 2 * 2:2], mixed[1:amount // 2 * 2:2]
    slack = jnp.minimum(tallies[donor] - 1, most - tallies[taker]) // 2
    slack = jnp.where((donor == sequence[0]) | (taker == sequence[0]) | (tallies[taker] == 0), 0, jnp.maximum(slack, 0))
    shifted = jax.random.randint(jax.random.fold_in(own, 4), (amount // 2,), 0, 1 << 20) % (slack + 1)
    tallies = tallies.at[donor].add(-shifted).at[taker].add(shifted)
    labels = jnp.searchsorted(jnp.cumsum(tallies), jnp.arange(rows * top), side="right").astype(jnp.int32)
    listing = labels.reshape(top, rows).T
    listing = listing[jax.random.permutation(jax.random.fold_in(own, 1), rows)]
    turn = jax.random.randint(jax.random.fold_in(own, 2), (rows, 1), 0, top)
    return jnp.take_along_axis(listing, (jnp.arange(top)[None, :] + turn) % top, axis=1)


def load_shares(number_of, total, limit, skew, full):
    weights = [(1 << 20) // math.isqrt(grade ** skew) + 1 for grade in range(1, number_of + 1)]
    largest = limit if full else min(limit, max(-(-total // number_of), total * weights[0] // sum(weights)))
    least = 1 if total - largest >= number_of - 1 else 0
    counts, spare = [largest] + [least] * (number_of - 1), total - largest - least * (number_of - 1)
    while spare > 0:
        movable = [i for i in range(1, number_of) if counts[i] < largest] or [i for i in range(1, number_of) if counts[i] < limit]
        mass, left = sum([weights[i] for i in movable]), spare
        for i in movable:
            more = min(limit - counts[i], max(1, left * weights[i] // mass), spare)
            counts[i] = counts[i] + more
            spare = spare - more
    return np.array(counts)


def setup_inputs(seed: int = 0) -> dict:
    streams_of = jax.random.split(jax.random.key(seed), 7)
    pixel_tiles = draw_pixel_tiles(jax.random.fold_in(streams_of[6], 71), 0)
    blend_source_keys = jax.random.split(jax.random.fold_in(streams_of[1], 1), BLENDS_ALL // BLEND_DEV)
    blend_source_turns = jax.random.permutation(jax.random.fold_in(streams_of[1], 3), BLENDS_ALL // BLEND_DEV)
    blend_source = jax.vmap(lambda own, number: shared_out(jax.random.fold_in(streams_of[1], 2), own, number, BLEND_DEV, N_DEV, FOOT, CAPACITY, 2))(blend_source_keys, blend_source_turns).reshape((BLENDS_ALL, FOOT))
    blend_slot = with_ends(jax.random.randint(streams_of[2], (BLENDS_ALL, FOOT), 0, TILE_DEV), jax.random.fold_in(streams_of[2], 1), 0, TILE_DEV - 1).astype(jnp.int32)
    component_count = with_ends(jax.random.randint(streams_of[3], (BLENDS_ALL,), COMPONENTS // 2, COMPONENTS + 1), jax.random.fold_in(streams_of[3], 1), COMPONENTS // 2, COMPONENTS).astype(jnp.int32)
    sed_start = jnp.clip(jnp.exp(math.log(0.5) - 2.306499 * jax.random.uniform(streams_of[4], (BLENDS_ALL, COMPONENTS, BANDS), jnp.float32) ** levels(streams_of[4], (BLENDS_ALL, COMPONENTS, BANDS), ((0, 32),), -0.2, 0.2)), 0.049804688, 0.5).astype(jnp.bfloat16)
    morph_start = jnp.clip(jnp.exp(math.log(0.5) - 3.224016 * jax.random.uniform(streams_of[5], (BLENDS_ALL, FOOT, COMPONENTS, PIX), jnp.float32) ** levels(streams_of[5], (BLENDS_ALL, FOOT, COMPONENTS, PIX), ((0, 32),), -0.2, 0.2)), 0.019897461, 0.5).astype(jnp.bfloat16)
    return dict(pixel_tiles=pixel_tiles, blend_source=blend_source, blend_slot=blend_slot, component_count=component_count, sed_start=sed_start, morph_start=morph_start)


def to_bf16(values):
    return lax.optimization_barrier(values.astype(jnp.bfloat16)).astype(jnp.float32)

def fit_block(blend_data, sed, morph, count):
    active = (jnp.arange(COMPONENTS, dtype=jnp.int32)[None, :] < count[:, None]).astype(jnp.float32)
    sed = sed.astype(jnp.float32) * active[:, :, None]
    morph = morph.astype(jnp.float32) * active[:, None, :, None]
    target = blend_data.astype(jnp.float32)
    for sweep in range(ITERS):
        misfit = to_bf16(jnp.einsum('nkb,nfkp->nfbp', sed, morph) - target)
        gram_matrix = jnp.einsum('nfkp,nfjp->nkj', morph, morph)
        lip_sed = jnp.sqrt(lax.optimization_barrier(jnp.sum(gram_matrix * gram_matrix, axis=(1, 2)))) + 1.0
        gradient = jnp.einsum('nfkp,nfbp->nkb', morph, misfit)
        sed = to_bf16(jnp.maximum(sed - gradient / lip_sed[:, None, None], 0.0) * active[:, :, None])
        misfit = to_bf16(jnp.einsum('nkb,nfkp->nfbp', sed, morph) - target)
        sed_gram = jnp.einsum('nkb,nkc->nbc', sed, sed)
        lip_morph = jnp.sqrt(lax.optimization_barrier(jnp.sum(sed_gram * sed_gram, axis=(1, 2)))) + 1.0
        grad_morph = jnp.einsum('nkb,nfbp->nfkp', sed, misfit)
        morph = to_bf16(jnp.maximum(morph - (grad_morph + 0.1) / lip_morph[:, None, None, None], 0.0) * active[:, None, :, None])
    model_out = jnp.einsum('nkb,nfkp->nfbp', sed, morph).astype(jnp.bfloat16)
    return (sed.astype(jnp.bfloat16), model_out)

def reference(pixel_tiles, blend_source, blend_slot, component_count, sed_start, morph_start):
    group_of = jnp.arange(BLENDS_ALL, dtype=jnp.int32) // BLENDS_G
    tile_index = (group_of[:, None] * TILES_G + blend_source * TILE_DEV + blend_slot).astype(jnp.int32)
    blocks = BLENDS_ALL // BLEND_DEV

    def visit(summed, inputs):
        rows, sed, morph, count = inputs
        blend_data = pixel_tiles[rows].astype(jnp.bfloat16)
        sed_new, model_out = fit_block(blend_data, sed, morph, count)
        summed = summed.at[rows.reshape(-1)].add(model_out.reshape(-1, BANDS, PIX).astype(jnp.float32))
        return (summed, sed_new)
    summed, sed_blocks = lax.scan(visit, jnp.zeros((TILES_ALL, BANDS, PIX), jnp.float32), (tile_index.reshape(blocks, BLEND_DEV, FOOT), sed_start.reshape(blocks, BLEND_DEV, COMPONENTS, BANDS), morph_start.reshape(blocks, BLEND_DEV, FOOT, COMPONENTS, PIX), component_count.reshape(blocks, BLEND_DEV)))
    residual = pixel_tiles - summed
    total_sq = jnp.sum(residual * residual)
    whitened = residual / jnp.sqrt(total_sq / float(TILES_ALL * BANDS * PIX) + 1e-06)
    return (whitened, sed_blocks.reshape(BLENDS_ALL, COMPONENTS, BANDS))
```

```python
import math

import jax
import jax.numpy as jnp
from jax import lax
from jax.sharding import PartitionSpec as P

ITERS = 2


def fit_block(blend_data, sed, morph, count):
    components = sed.shape[1]
    active = (jnp.arange(components, dtype=jnp.int32)[None, :] < count[:, None]).astype(jnp.float32)
    sed = (sed.astype(jnp.float32) * active[:, :, None]).astype(jnp.bfloat16)
    morph = morph * active[:, None, :, None].astype(jnp.bfloat16)
    target = blend_data.astype(jnp.float32)
    for sweep in range(ITERS):
        model = jnp.einsum("nkb,nfkp->nfbp", sed, morph, preferred_element_type=jnp.float32)
        misfit = (model - target).astype(jnp.bfloat16)
        gram_matrix = jnp.einsum("nfkp,nfjp->nkj", morph, morph, preferred_element_type=jnp.float32)
        lip_sed = jnp.sqrt(jnp.sum(gram_matrix * gram_matrix, axis=(1, 2))) + 1.0
        gradient = jnp.einsum("nfkp,nfbp->nkb", morph, misfit, preferred_element_type=jnp.float32)
        sed = (
            jnp.maximum(sed.astype(jnp.float32) - gradient / lip_sed[:, None, None], 0.0)
            * active[:, :, None]
        ).astype(jnp.bfloat16)
        model = jnp.einsum("nkb,nfkp->nfbp", sed, morph, preferred_element_type=jnp.float32)
        misfit = (model - target).astype(jnp.bfloat16)
        sed_gram = jnp.einsum("nkb,nkc->nbc", sed, sed, preferred_element_type=jnp.float32)
        lip_morph = jnp.sqrt(jnp.sum(sed_gram * sed_gram, axis=(1, 2))) + 1.0
        grad_morph = jnp.einsum("nkb,nfbp->nfkp", sed, misfit, preferred_element_type=jnp.float32)
        morph = (
            jnp.maximum(morph - (grad_morph + 0.1) / lip_morph[:, None, None, None], 0.0)
            * active[:, None, :, None]
        ).astype(jnp.bfloat16)
    model_out = jnp.einsum("nkb,nfkp->nfbp", sed, morph, preferred_element_type=jnp.float32).astype(
        jnp.bfloat16
    )
    return (sed, morph, model_out)


def on_device(pixel_tiles, blend_source, blend_slot, component_count, sed_start, morph_start):
    peer_count = lax.axis_size("dev")
    blend_rows, footprint = blend_source.shape
    entries = blend_rows * footprint
    capacity = max(2, (entries + peer_count - 1) // peer_count)
    tile_rows, bands, pixels = pixel_tiles.shape
    sources = blend_source.reshape(entries)
    one_hot = (sources[:, None] == jnp.arange(peer_count, dtype=jnp.int32)[None, :]).astype(
        jnp.int32
    )
    ranking = jnp.sum((jnp.cumsum(one_hot, axis=0) - 1) * one_hot, axis=1)
    placing = sources * capacity + ranking
    asking = (
        jnp.zeros((peer_count * capacity,), jnp.int32)
        .at[placing]
        .set(blend_slot.reshape(entries) + 1)
    )
    wanted = lax.all_to_all(
        asking.reshape(peer_count, capacity), "dev", split_axis=0, concat_axis=0, tiled=True
    )
    source_rows = jnp.maximum(wanted - 1, 0).reshape(-1)
    filled = (wanted > 0).reshape(-1)
    outgoing = jnp.where(filled[:, None, None], pixel_tiles[source_rows], 0.0).astype(jnp.bfloat16)
    arrived = lax.all_to_all(
        outgoing.reshape(peer_count, capacity, bands, pixels),
        "dev",
        split_axis=0,
        concat_axis=0,
        tiled=True,
    )
    blend_data = arrived.reshape(peer_count * capacity, bands, pixels)[placing].reshape(
        blend_rows, footprint, bands, pixels
    )
    block_size = math.gcd(blend_rows, 8)
    groups = blend_rows // block_size

    def in_blocks(array):
        return array.reshape((groups, block_size) + array.shape[1:])

    sed_blocks, morph_blocks, model_blocks = lax.map(
        lambda inputs: fit_block(*inputs),
        (
            in_blocks(blend_data),
            in_blocks(sed_start),
            in_blocks(morph_start),
            in_blocks(component_count),
        ),
    )
    sed_final = sed_blocks.reshape(sed_start.shape)
    models = model_blocks.reshape(entries, bands, pixels)
    outbound = (
        jnp.zeros((peer_count * capacity, bands, pixels), jnp.bfloat16).at[placing].set(models)
    )
    returned = lax.all_to_all(
        outbound.reshape(peer_count, capacity, bands, pixels),
        "dev",
        split_axis=0,
        concat_axis=0,
        tiled=True,
    )
    returned = returned.reshape(peer_count * capacity, bands * pixels)
    selector = (
        (source_rows[None, :] == jnp.arange(tile_rows, dtype=jnp.int32)[:, None]) & filled[None, :]
    ).astype(jnp.bfloat16)
    summed = jnp.dot(selector, returned, preferred_element_type=jnp.float32).reshape(
        tile_rows, bands, pixels
    )
    residual = pixel_tiles - summed
    everyone = lax.axis_size("grp") * peer_count
    partial = jnp.broadcast_to(jnp.sum(residual * residual), (everyone, 1, 128))
    partials = lax.all_to_all(partial, ("grp", "dev"), split_axis=0, concat_axis=0, tiled=True)
    total_sq = jnp.sum(partials[:, 0, 0])
    pixel_count = float(residual.size * lax.axis_size("grp") * peer_count)
    whitened = residual / jnp.sqrt(total_sq / pixel_count + 1e-06)
    return (whitened, sed_final)


def solution(mesh):
    placed = (
        P(("grp", "dev"), None, None),
        P(("grp", "dev"), None),
        P(("grp", "dev"), None),
        P(("grp", "dev")),
        P(("grp", "dev"), None, None),
        P(("grp", "dev"), None, None, None),
    )
    return jax.shard_map(
        on_device,
        mesh=mesh,
        in_specs=placed,
        out_specs=(P(("grp", "dev"), None, None), P(("grp", "dev"), None, None)),
        check_vma=False,
    )
```

```python
import functools
import math

import jax
import jax.numpy as jnp
from jax import lax
from jax.experimental import pallas as pl
from jax.experimental.pallas import tpu as pltpu
from jax.sharding import PartitionSpec as P

ITERS = 2
LANES = 8
F32 = jnp.float32
BF16 = jnp.bfloat16


def dot(left, right, left_dim, right_dim):
    return lax.dot_general(
        left, right, (((left_dim,), (right_dim,)), ((), ())), preferred_element_type=F32
    )


def inverse_lip(squares, components):
    rows, width = squares.shape
    total = jnp.sum(
        jnp.sum(squares.reshape(rows // components, components, width), axis=1),
        axis=1,
        keepdims=True,
    )
    inverse = 1.0 / (jnp.sqrt(total) + 1.0)
    return jnp.concatenate(
        [jnp.broadcast_to(inverse[n : n + 1], (components, 1)) for n in range(rows // components)],
        axis=0,
    )


def place_kernel(source_ref, slot_ref, asking_ref, placing_ref):
    peers, capacity = asking_ref.shape
    entries = source_ref.shape[1]
    peer = lax.broadcasted_iota(jnp.int32, (peers, entries), 0)
    named = peer == source_ref[...]
    before = lax.broadcasted_iota(jnp.int32, (entries, entries), 0)
    after = lax.broadcasted_iota(jnp.int32, (entries, entries), 1)
    upto = (before <= after).astype(F32).astype(BF16)
    rank = dot(named.astype(F32).astype(BF16), upto, 1, 0).astype(jnp.int32) - 1
    placing_ref[...] = jnp.sum(jnp.where(named, peer * capacity + rank, 0), axis=0, keepdims=True)
    value = jnp.broadcast_to(slot_ref[...] + 1, (peers, entries))
    for s in range(capacity):
        hit = jnp.where(named & (rank == s), value, 0)
        asking_ref[:, s : s + 1] = jnp.sum(hit, axis=1, keepdims=True)


def fit_kernel(
    count_ref, placing_ref, arrived_ref, sed_ref, morph_ref, sed_out_ref, out_ref,
    x_ref, mask_ref, data_ref, model_ref, *, units,
):
    step = pl.program_id(0)
    bands, slots, pixels = arrived_ref.shape
    entries = placing_ref.shape[1]
    footprint, components = morph_ref.shape[1:3]
    blends = entries // footprint
    rows = LANES * components
    cols = LANES * bands
    depth = x_ref.shape[1]

    def permutation():
        slot = lax.broadcasted_iota(jnp.int32, (slots, entries), 0)
        return (slot == placing_ref[...]).astype(F32).astype(BF16)

    @pl.when(step == 0)
    def _():
        chosen = permutation()
        for b in range(bands):
            data_ref[b] = dot(chosen, arrived_ref[b], 0, 0)
        lane = lax.broadcasted_iota(jnp.int32, (components, depth), 1)
        for n in range(LANES):
            own = (lane >= components * n) & (lane < components * (n + 1))
            side = (lane >= rows) & (lane < rows + cols) & (((lane - rows) & (LANES - 1)) == n)
            mask_ref[components * n : components * (n + 1), :] = (own | side).astype(F32)

    mask = mask_ref[...]
    in_gram = lax.broadcasted_iota(jnp.int32, (rows, depth), 1) < rows
    eye_row = lax.broadcasted_iota(jnp.int32, (depth - rows, cols), 0)
    eye_col = lax.broadcasted_iota(jnp.int32, (depth - rows, cols), 1)
    minus_eye = jnp.where(eye_row == eye_col, -1.0, 0.0)
    column = lax.broadcasted_iota(jnp.int32, (components, cols), 1)
    component = lax.broadcasted_iota(jnp.int32, (components, cols), 0)
    level = lax.broadcasted_iota(jnp.int32, (components, footprint * pixels), 0)
    seds = []
    for u in range(units):
        first = (step * units + u) * LANES
        counts = [count_ref[first + n] for n in range(LANES)]
        start = sed_ref[u].astype(F32)
        seds.append(
            jnp.concatenate(
                [
                    jnp.where(((column & (LANES - 1)) == n) & (component < counts[n]), start, 0.0)
                    for n in range(LANES)
                ],
                axis=0,
            )
        )
        morph = jnp.concatenate(
            [
                jnp.where(
                    level < counts[n],
                    jnp.concatenate(
                        [morph_ref[u * LANES + n, f].astype(F32) for f in range(footprint)], axis=1
                    ),
                    0.0,
                )
                for n in range(LANES)
            ],
            axis=0,
        )
        x_ref[u, 0:rows, :] = morph.astype(BF16)
        data = jnp.concatenate(
            [
                jnp.concatenate(
                    [
                        data_ref[b, pl.ds(pl.multiple_of(f * blends + first, LANES), LANES), :]
                        for f in range(footprint)
                    ],
                    axis=1,
                )
                for b in range(bands)
            ]
            + [jnp.zeros((depth - rows - cols, footprint * pixels), F32)],
            axis=0,
        )
        x_ref[u, rows:depth, :] = data.astype(BF16)
    for sweep in range(ITERS):
        grams = [dot(x_ref[u, 0:rows, :], x_ref[u], 1, 1) * mask for u in range(units)]
        for u in range(units):
            inverse = inverse_lip(jnp.where(in_gram, grams[u] * grams[u], 0.0), components)
            right = jnp.concatenate([seds[u], minus_eye], axis=0).astype(BF16)
            high = grams[u].astype(BF16)
            low = (grams[u] - high.astype(F32)).astype(BF16)
            gradient = dot(high, right, 1, 0) + dot(low, right, 1, 0)
            seds[u] = jnp.maximum(seds[u] - gradient * inverse, 0.0).astype(BF16).astype(F32)
        for u in range(units):
            right = jnp.concatenate([seds[u], minus_eye], axis=0).astype(BF16)
            left = dot(seds[u].astype(BF16), right, 1, 1)
            inverse = inverse_lip(jnp.where(in_gram, left * left, 0.0), components)
            gradient = dot(left.astype(BF16), x_ref[u], 1, 0)
            morph = x_ref[u, 0:rows, :].astype(F32)
            morph = jnp.maximum(morph - (gradient + 0.1) * inverse, 0.0)
            x_ref[u, 0:rows, :] = morph.astype(BF16)
    for u in range(units):
        first = (step * units + u) * LANES
        model = dot(seds[u].astype(BF16), x_ref[u, 0:rows, :], 0, 0)
        for b in range(bands):
            for f in range(footprint):
                model_ref[b, pl.ds(pl.multiple_of(f * blends + first, LANES), LANES), :] = model[
                    LANES * b : LANES * (b + 1), pixels * f : pixels * (f + 1)
                ]
        sed_out_ref[u] = jnp.sum(seds[u].reshape(LANES, components, cols), axis=0).astype(BF16)

    @pl.when(step == pl.num_programs(0) - 1)
    def _():
        chosen = permutation()
        for b in range(bands):
            out_ref[b] = dot(chosen, model_ref[b].astype(BF16), 1, 0).astype(BF16)


def on_device(pixel_tiles, blend_source, blend_slot, component_count, sed_start, morph_start):
    peer_count = lax.axis_size("dev")
    blend_rows, footprint = blend_source.shape
    components, bands = sed_start.shape[1:]
    entries = blend_rows * footprint
    capacity = max(2, (entries + peer_count - 1) // peer_count)
    slots = peer_count * capacity
    tile_rows, bands, pixels = pixel_tiles.shape
    asking, placing = pl.pallas_call(
        place_kernel,
        out_shape=(
            jax.ShapeDtypeStruct((peer_count, capacity), jnp.int32),
            jax.ShapeDtypeStruct((1, entries), jnp.int32),
        ),
        name="place",
    )(blend_source.T.reshape(1, entries), blend_slot.T.reshape(1, entries))
    wanted = lax.all_to_all(asking, "dev", split_axis=0, concat_axis=0, tiled=True).reshape(slots)
    selector = (
        wanted[None, :] == jnp.arange(1, tile_rows + 1, dtype=jnp.int32)[:, None]
    ).astype(BF16)
    outgoing = jnp.einsum(
        "ts,tbp->bsp", selector, pixel_tiles.astype(BF16), preferred_element_type=F32
    ).astype(BF16)

    def exchange(tiles):
        wire = tiles.reshape(bands, peer_count, capacity, pixels).transpose(1, 2, 0, 3)
        moved = lax.all_to_all(wire, "dev", split_axis=0, concat_axis=0, tiled=True)
        return moved.transpose(2, 0, 1, 3).reshape(bands, slots, pixels)

    arrived = exchange(outgoing)
    groups = blend_rows // LANES
    units = math.gcd(groups, 2)
    rows, cols = LANES * components, LANES * bands
    depth = -(-(rows + cols) // 128) * 128
    sed_in = (
        sed_start.reshape(groups, LANES, components, bands)
        .transpose(0, 2, 3, 1)
        .reshape(groups, components, cols)
    )
    sed_blocks, models = pl.pallas_call(
        functools.partial(fit_kernel, units=units),
        grid=(groups // units,),
        in_specs=[
            pl.BlockSpec(memory_space=pltpu.SMEM),
            pl.BlockSpec((1, entries), lambda i: (0, 0)),
            pl.BlockSpec((bands, slots, pixels), lambda i: (0, 0, 0)),
            pl.BlockSpec((units, components, cols), lambda i: (i, 0, 0)),
            pl.BlockSpec((units * LANES, footprint, components, pixels), lambda i: (i, 0, 0, 0)),
        ],
        out_specs=[
            pl.BlockSpec((units, components, cols), lambda i: (i, 0, 0)),
            pl.BlockSpec((bands, slots, pixels), lambda i: (0, 0, 0)),
        ],
        out_shape=(
            jax.ShapeDtypeStruct((groups, components, cols), BF16),
            jax.ShapeDtypeStruct((bands, slots, pixels), BF16),
        ),
        scratch_shapes=[
            pltpu.VMEM((units, depth, footprint * pixels), BF16),
            pltpu.VMEM((rows, depth), F32),
            pltpu.VMEM((bands, entries, pixels), F32),
            pltpu.VMEM((bands, entries, pixels), F32),
        ],
        compiler_params=pltpu.CompilerParams(dimension_semantics=("arbitrary",)),
        name="fit",
    )(component_count, placing, arrived, sed_in, morph_start)
    sed_final = (
        sed_blocks.reshape(groups, components, bands, LANES)
        .transpose(0, 3, 1, 2)
        .reshape(sed_start.shape)
    )
    returned = exchange(models)
    summed = jnp.einsum("ts,bsp->tbp", selector, returned, preferred_element_type=F32)
    residual = pixel_tiles - summed
    everyone = lax.axis_size("grp") * peer_count
    partial = jnp.broadcast_to(jnp.sum(residual * residual), (everyone, 1, 128))
    partials = lax.all_to_all(partial, ("grp", "dev"), split_axis=0, concat_axis=0, tiled=True)
    total_sq = jnp.sum(partials[:, 0, 0])
    pixel_count = float(residual.size * everyone)
    whitened = residual / jnp.sqrt(total_sq / pixel_count + 1e-06)
    return (whitened, sed_final)


def solution(mesh):
    placed = (
        P(("grp", "dev"), None, None),
        P(("grp", "dev"), None),
        P(("grp", "dev"), None),
        P(("grp", "dev")),
        P(("grp", "dev"), None, None),
        P(("grp", "dev"), None, None, None),
    )
    return jax.shard_map(
        on_device,
        mesh=mesh,
        in_specs=placed,
        out_specs=(P(("grp", "dev"), None, None), P(("grp", "dev"), None, None)),
        check_vma=False,
    )
```

```python
import functools
import math

import jax
import jax.numpy as jnp
from jax import lax
from jax.experimental import pallas as pl
from jax.experimental.pallas import tpu as pltpu
from jax.sharding import PartitionSpec as P

ITERS = 2
LANES = 8
F32 = jnp.float32
BF16 = jnp.bfloat16


def dot(left, right, left_dim, right_dim):
    return lax.dot_general(
        left, right, (((left_dim,), (right_dim,)), ((), ())), preferred_element_type=F32
    )


def inverse_lip(squares, components):
    rows, width = squares.shape
    total = jnp.sum(
        jnp.sum(squares.reshape(rows // components, components, width), axis=1),
        axis=1,
        keepdims=True,
    )
    inverse = 1.0 / (jnp.sqrt(total) + 1.0)
    return jnp.concatenate(
        [jnp.broadcast_to(inverse[n : n + 1], (components, 1)) for n in range(rows // components)],
        axis=0,
    )


def place_kernel(source_ref, slot_ref, asking_ref, placing_ref):
    peers, capacity = asking_ref.shape
    footprint, blends = source_ref.shape
    entries = footprint * blends
    source = jnp.concatenate([source_ref[f : f + 1, :] for f in range(footprint)], axis=1)
    slot = jnp.concatenate([slot_ref[f : f + 1, :] for f in range(footprint)], axis=1)
    peer = lax.broadcasted_iota(jnp.int32, (peers, entries), 0)
    named = peer == source
    before = lax.broadcasted_iota(jnp.int32, (entries, entries), 0)
    after = lax.broadcasted_iota(jnp.int32, (entries, entries), 1)
    upto = (before <= after).astype(F32).astype(BF16)
    rank = dot(named.astype(F32).astype(BF16), upto, 1, 0).astype(jnp.int32) - 1
    placing_ref[...] = jnp.sum(jnp.where(named, peer * capacity + rank, 0), axis=0, keepdims=True)
    value = jnp.broadcast_to(slot + 1, (peers, entries))
    for s in range(capacity):
        hit = jnp.where(named & (rank == s), value, 0)
        asking_ref[:, s : s + 1] = jnp.sum(hit, axis=1, keepdims=True)


def read_band(ref, b):
    if len(ref.shape) == 3:
        return ref[b]
    peers, _, capacity, pixels = ref.shape
    return ref[:, b].astype(F32).reshape(peers * capacity, pixels).astype(BF16)


def write_band(ref, b, value):
    if len(ref.shape) == 3:
        ref[b] = value.astype(BF16)
    else:
        peers, _, capacity, pixels = ref.shape
        ref[:, b] = value.reshape(peers, capacity, pixels).astype(BF16)


def send_kernel(wanted_ref, tiles_ref, selector_ref, out_ref):
    peers, capacity = wanted_ref.shape
    bands, tile_rows, _ = tiles_ref.shape
    slots = peers * capacity
    lane = lax.broadcasted_iota(jnp.int32, (capacity, slots), 1)
    within = lax.broadcasted_iota(jnp.int32, (capacity, slots), 0)
    spread = (lane % capacity == within).astype(F32)
    wide = lax.dot_general(
        wanted_ref[...].astype(F32), spread, (((1,), (0,)), ((), ())),
        precision=lax.Precision.HIGHEST, preferred_element_type=F32,
    )
    peer = lax.broadcasted_iota(jnp.int32, (peers, slots), 0)
    column = lax.broadcasted_iota(jnp.int32, (peers, slots), 1)
    mine = (column >= peer * capacity) & (column < (peer + 1) * capacity)
    wanted = jnp.sum(jnp.where(mine, wide, 0.0), axis=0, keepdims=True).astype(jnp.int32)
    tile = lax.broadcasted_iota(jnp.int32, (tile_rows, slots), 0) + 1
    selector = (tile == wanted).astype(F32).astype(BF16)
    selector_ref[...] = selector
    for b in range(bands):
        write_band(out_ref, b, dot(selector, tiles_ref[b].astype(BF16), 0, 0))


def residual_kernel(selector_ref, tiles_ref, returned_ref, residual_ref, partial_ref):
    bands = tiles_ref.shape[0]
    selector = selector_ref[...]
    squares = jnp.zeros(tiles_ref.shape[1:], F32)
    for b in range(bands):
        residual = tiles_ref[b] - dot(selector, read_band(returned_ref, b), 1, 0)
        residual_ref[b] = residual
        squares = squares + residual * residual
    partial_ref[...] = jnp.broadcast_to(
        jnp.sum(jnp.sum(squares, axis=0, keepdims=True), axis=1, keepdims=True)[None],
        partial_ref.shape,
    )


def fit_kernel(
    count_ref, placing_ref, arrived_ref, sed_ref, morph_ref, sed_out_ref, out_ref,
    x_ref, mask_ref, data_ref, model_ref, *, units,
):
    step = pl.program_id(0)
    bands, entries, pixels = data_ref.shape
    slots = math.prod(arrived_ref.shape) // (bands * pixels)
    footprint, components = morph_ref.shape[1:3]
    blends = entries // footprint
    rows = LANES * components
    cols = LANES * bands
    depth = x_ref.shape[1]

    def permutation():
        slot = lax.broadcasted_iota(jnp.int32, (slots, entries), 0)
        return (slot == placing_ref[...]).astype(F32).astype(BF16)

    @pl.when(step == 0)
    def _():
        chosen = permutation()
        for b in range(bands):
            data_ref[b] = dot(chosen, read_band(arrived_ref, b), 0, 0)
        lane = lax.broadcasted_iota(jnp.int32, (components, depth), 1)
        for n in range(LANES):
            own = (lane >= components * n) & (lane < components * (n + 1))
            side = (lane >= rows) & (lane < rows + cols) & (((lane - rows) & (LANES - 1)) == n)
            mask_ref[components * n : components * (n + 1), :] = (own | side).astype(F32)

    mask = mask_ref[...]
    in_gram = lax.broadcasted_iota(jnp.int32, (rows, depth), 1) < rows
    eye_row = lax.broadcasted_iota(jnp.int32, (depth - rows, cols), 0)
    eye_col = lax.broadcasted_iota(jnp.int32, (depth - rows, cols), 1)
    minus_eye = jnp.where(eye_row == eye_col, -1.0, 0.0)
    column = lax.broadcasted_iota(jnp.int32, (components, cols), 1)
    component = lax.broadcasted_iota(jnp.int32, (components, cols), 0)
    level = lax.broadcasted_iota(jnp.int32, (components, footprint * pixels), 0)
    seds = []
    for u in range(units):
        first = (step * units + u) * LANES
        counts = [count_ref[first + n] for n in range(LANES)]
        start = sed_ref[u].astype(F32)
        seds.append(
            jnp.concatenate(
                [
                    jnp.where(((column & (LANES - 1)) == n) & (component < counts[n]), start, 0.0)
                    for n in range(LANES)
                ],
                axis=0,
            )
        )
        morph = jnp.concatenate(
            [
                jnp.where(
                    level < counts[n],
                    jnp.concatenate(
                        [morph_ref[u * LANES + n, f].astype(F32) for f in range(footprint)], axis=1
                    ),
                    0.0,
                )
                for n in range(LANES)
            ],
            axis=0,
        )
        x_ref[u, 0:rows, :] = morph.astype(BF16)
        data = jnp.concatenate(
            [
                jnp.concatenate(
                    [
                        data_ref[b, pl.ds(pl.multiple_of(f * blends + first, LANES), LANES), :]
                        for f in range(footprint)
                    ],
                    axis=1,
                )
                for b in range(bands)
            ]
            + [jnp.zeros((depth - rows - cols, footprint * pixels), F32)],
            axis=0,
        )
        x_ref[u, rows:depth, :] = data.astype(BF16)
    for sweep in range(ITERS):
        grams = [dot(x_ref[u, 0:rows, :], x_ref[u], 1, 1) * mask for u in range(units)]
        for u in range(units):
            inverse = inverse_lip(jnp.where(in_gram, grams[u] * grams[u], 0.0), components)
            right = jnp.concatenate([seds[u], minus_eye], axis=0).astype(BF16)
            high = grams[u].astype(BF16)
            low = (grams[u] - high.astype(F32)).astype(BF16)
            gradient = dot(high, right, 1, 0) + dot(low, right, 1, 0)
            seds[u] = jnp.maximum(seds[u] - gradient * inverse, 0.0).astype(BF16).astype(F32)
        for u in range(units):
            right = jnp.concatenate([seds[u], minus_eye], axis=0).astype(BF16)
            left = dot(seds[u].astype(BF16), right, 1, 1)
            inverse = inverse_lip(jnp.where(in_gram, left * left, 0.0), components)
            gradient = dot(left.astype(BF16), x_ref[u], 1, 0)
            morph = x_ref[u, 0:rows, :].astype(F32)
            morph = jnp.maximum(morph - (gradient + 0.1) * inverse, 0.0)
            x_ref[u, 0:rows, :] = morph.astype(BF16)
    for u in range(units):
        first = (step * units + u) * LANES
        model = dot(seds[u].astype(BF16), x_ref[u, 0:rows, :], 0, 0)
        for b in range(bands):
            for f in range(footprint):
                model_ref[b, pl.ds(pl.multiple_of(f * blends + first, LANES), LANES), :] = model[
                    LANES * b : LANES * (b + 1), pixels * f : pixels * (f + 1)
                ]
        sed_out_ref[u] = jnp.sum(seds[u].reshape(LANES, components, cols), axis=0).astype(BF16)

    @pl.when(step == pl.num_programs(0) - 1)
    def _():
        chosen = permutation()
        for b in range(bands):
            write_band(out_ref, b, dot(chosen, model_ref[b].astype(BF16), 1, 0))


def on_device(pixel_tiles, blend_source, blend_slot, component_count, sed_start, morph_start):
    peer_count = lax.axis_size("dev")
    blend_rows, footprint = blend_source.shape
    components, bands = sed_start.shape[1:]
    entries = blend_rows * footprint
    capacity = max(2, (entries + peer_count - 1) // peer_count)
    slots = peer_count * capacity
    tile_rows, bands, pixels = pixel_tiles.shape
    asking, placing = pl.pallas_call(
        place_kernel,
        out_shape=(
            jax.ShapeDtypeStruct((peer_count, capacity), jnp.int32),
            jax.ShapeDtypeStruct((1, entries), jnp.int32),
        ),
        compiler_params=pltpu.CompilerParams(vmem_limit_bytes=16 * 2**20),
        name="place",
    )(blend_source.T, blend_slot.T)
    wanted = lax.all_to_all(asking, "dev", split_axis=0, concat_axis=0, tiled=True)
    direct = capacity % 8 == 0
    banded = (bands, slots, pixels)
    tile_shape = (peer_count, bands, capacity, pixels) if direct else banded
    tiles = pixel_tiles.transpose(1, 0, 2)
    selector, outgoing = pl.pallas_call(
        send_kernel,
        out_shape=(
            jax.ShapeDtypeStruct((tile_rows, slots), BF16),
            jax.ShapeDtypeStruct(tile_shape, BF16),
        ),
        compiler_params=pltpu.CompilerParams(vmem_limit_bytes=16 * 2**20),
        name="send",
    )(wanted, tiles)

    def exchange(wire):
        if not direct:
            wire = wire.reshape(bands, peer_count, capacity, pixels).transpose(1, 2, 0, 3)
        moved = lax.all_to_all(wire, "dev", split_axis=0, concat_axis=0, tiled=True)
        return moved if direct else moved.transpose(2, 0, 1, 3).reshape(banded)

    arrived = exchange(outgoing)
    groups = blend_rows // LANES
    units = math.gcd(groups, 2)
    rows, cols = LANES * components, LANES * bands
    depth = -(-(rows + cols) // 128) * 128
    sed_in = (
        sed_start.reshape(groups, LANES, components, bands)
        .transpose(0, 2, 3, 1)
        .reshape(groups, components, cols)
    )
    sed_blocks, models = pl.pallas_call(
        functools.partial(fit_kernel, units=units),
        grid=(groups // units,),
        in_specs=[
            pl.BlockSpec(memory_space=pltpu.SMEM),
            pl.BlockSpec(memory_space=pltpu.VMEM),
            pl.BlockSpec(memory_space=pltpu.VMEM),
            pl.BlockSpec((units, components, cols), lambda i: (i, 0, 0)),
            pl.BlockSpec((units * LANES, footprint, components, pixels), lambda i: (i, 0, 0, 0)),
        ],
        out_specs=[
            pl.BlockSpec((units, components, cols), lambda i: (i, 0, 0)),
            pl.BlockSpec(tile_shape, lambda i: (0,) * len(tile_shape)),
        ],
        out_shape=(
            jax.ShapeDtypeStruct((groups, components, cols), BF16),
            jax.ShapeDtypeStruct(tile_shape, BF16),
        ),
        scratch_shapes=[
            pltpu.VMEM((units, depth, footprint * pixels), BF16),
            pltpu.VMEM((rows, depth), F32),
            pltpu.VMEM((bands, entries, pixels), F32),
            pltpu.VMEM((bands, entries, pixels), F32),
        ],
        compiler_params=pltpu.CompilerParams(
            dimension_semantics=("arbitrary",), vmem_limit_bytes=24 * 2**20
        ),
        name="fit",
    )(component_count, placing, arrived, sed_in, morph_start)
    sed_final = (
        sed_blocks.reshape(groups, components, bands, LANES)
        .transpose(0, 3, 1, 2)
        .reshape(sed_start.shape)
    )
    returned = exchange(models)
    everyone = lax.axis_size("grp") * peer_count
    residual, partial = pl.pallas_call(
        residual_kernel,
        out_shape=(
            jax.ShapeDtypeStruct((bands, tile_rows, pixels), F32),
            jax.ShapeDtypeStruct((everyone, 1, 128), F32),
        ),
        in_specs=[pl.BlockSpec(memory_space=pltpu.VMEM)] * 3,
        out_specs=[pl.BlockSpec(memory_space=pltpu.VMEM)] * 2,
        compiler_params=pltpu.CompilerParams(vmem_limit_bytes=16 * 2**20),
        name="residual",
    )(selector, tiles, returned)
    partials = lax.all_to_all(partial, ("grp", "dev"), split_axis=0, concat_axis=0, tiled=True)
    total_sq = jnp.sum(partials[:, 0, 0])
    pixel_count = float(residual.size * everyone)
    whitened = residual / jnp.sqrt(total_sq / pixel_count + 1e-06)
    return (whitened.transpose(1, 0, 2), sed_final)


def solution(mesh):
    placed = (
        P(("grp", "dev"), None, None),
        P(("grp", "dev"), None),
        P(("grp", "dev"), None),
        P(("grp", "dev")),
        P(("grp", "dev"), None, None),
        P(("grp", "dev"), None, None, None),
    )
    return jax.shard_map(
        on_device,
        mesh=mesh,
        in_specs=placed,
        out_specs=(P(("grp", "dev"), None, None), P(("grp", "dev"), None, None)),
        check_vma=False,
    )
```

```python
import functools
import math

import jax
import jax.numpy as jnp
from jax import lax
from jax.experimental import pallas as pl
from jax.experimental.pallas import tpu as pltpu
from jax.sharding import PartitionSpec as P

ITERS = 2
LANES = 8
F32 = jnp.float32
BF16 = jnp.bfloat16


def dot(left, right, left_dim, right_dim):
    return lax.dot_general(
        left, right, (((left_dim,), (right_dim,)), ((), ())), preferred_element_type=F32
    )


def inverse_lip(squares, components):
    rows, width = squares.shape
    total = jnp.sum(
        jnp.sum(squares.reshape(rows // components, components, width), axis=1),
        axis=1,
        keepdims=True,
    )
    inverse = 1.0 / (jnp.sqrt(total) + 1.0)
    return jnp.concatenate(
        [jnp.broadcast_to(inverse[n : n + 1], (components, 1)) for n in range(rows // components)],
        axis=0,
    )


def place_kernel(source_ref, slot_ref, asking_ref, placing_ref):
    peers, capacity = asking_ref.shape
    footprint, blends = source_ref.shape
    entries = footprint * blends
    source = jnp.concatenate([source_ref[f : f + 1, :] for f in range(footprint)], axis=1)
    slot = jnp.concatenate([slot_ref[f : f + 1, :] for f in range(footprint)], axis=1)
    peer = lax.broadcasted_iota(jnp.int32, (peers, entries), 0)
    named = peer == source
    before = lax.broadcasted_iota(jnp.int32, (entries, entries), 0)
    after = lax.broadcasted_iota(jnp.int32, (entries, entries), 1)
    upto = (before <= after).astype(F32).astype(BF16)
    rank = dot(named.astype(F32).astype(BF16), upto, 1, 0).astype(jnp.int32) - 1
    placing_ref[...] = jnp.sum(jnp.where(named, peer * capacity + rank, 0), axis=0, keepdims=True)
    value = jnp.broadcast_to(slot + 1, (peers, entries))
    for s in range(capacity):
        hit = jnp.where(named & (rank == s), value, 0)
        asking_ref[:, s : s + 1] = jnp.sum(hit, axis=1, keepdims=True)


def read_band(ref, b):
    if len(ref.shape) == 3:
        return ref[b]
    peers, _, capacity, pixels = ref.shape
    return ref[:, b].astype(F32).reshape(peers * capacity, pixels).astype(BF16)


def write_band(ref, b, value):
    if len(ref.shape) == 3:
        ref[b] = value.astype(BF16)
    else:
        peers, _, capacity, pixels = ref.shape
        ref[:, b] = value.reshape(peers, capacity, pixels).astype(BF16)


def send_kernel(wanted_ref, tiles_ref, selector_ref, out_ref):
    peers, capacity = wanted_ref.shape
    bands, tile_rows, _ = tiles_ref.shape
    slots = peers * capacity
    lane = lax.broadcasted_iota(jnp.int32, (capacity, slots), 1)
    within = lax.broadcasted_iota(jnp.int32, (capacity, slots), 0)
    spread = (lane % capacity == within).astype(F32)
    wide = lax.dot_general(
        wanted_ref[...].astype(F32), spread, (((1,), (0,)), ((), ())),
        precision=lax.Precision.HIGHEST, preferred_element_type=F32,
    )
    peer = lax.broadcasted_iota(jnp.int32, (peers, slots), 0)
    column = lax.broadcasted_iota(jnp.int32, (peers, slots), 1)
    mine = (column >= peer * capacity) & (column < (peer + 1) * capacity)
    wanted = jnp.sum(jnp.where(mine, wide, 0.0), axis=0, keepdims=True).astype(jnp.int32)
    tile = lax.broadcasted_iota(jnp.int32, (tile_rows, slots), 0) + 1
    selector = (tile == wanted).astype(F32).astype(BF16)
    selector_ref[...] = selector
    for b in range(bands):
        write_band(out_ref, b, dot(selector, tiles_ref[b].astype(BF16), 0, 0))


def residual_kernel(selector_ref, tiles_ref, returned_ref, residual_ref, partial_ref):
    bands = tiles_ref.shape[0]
    selector = selector_ref[...]
    squares = jnp.zeros(tiles_ref.shape[1:], F32)
    for b in range(bands):
        residual = tiles_ref[b] - dot(selector, read_band(returned_ref, b), 1, 0)
        residual_ref[b] = residual
        squares = squares + residual * residual
    partial_ref[...] = jnp.broadcast_to(
        jnp.sum(jnp.sum(squares, axis=0, keepdims=True), axis=1, keepdims=True)[None],
        partial_ref.shape,
    )


def fit_kernel(
    count_ref, placing_ref, arrived_ref, sed_ref, morph_ref, sed_out_ref, out_ref,
    x_ref, mask_ref, data_ref, model_ref, *, units,
):
    step = pl.program_id(0)
    bands, entries, pixels = data_ref.shape
    slots = math.prod(arrived_ref.shape) // (bands * pixels)
    footprint, components = morph_ref.shape[1:3]
    blends = entries // footprint
    rows = LANES * components
    cols = LANES * bands
    depth = x_ref.shape[1]

    def permutation():
        slot = lax.broadcasted_iota(jnp.int32, (slots, entries), 0)
        return (slot == placing_ref[...]).astype(F32).astype(BF16)

    @pl.when(step == 0)
    def _():
        chosen = permutation()
        for b in range(bands):
            data_ref[b] = dot(chosen, read_band(arrived_ref, b), 0, 0)
        lane = lax.broadcasted_iota(jnp.int32, (components, depth), 1)
        for n in range(LANES):
            own = (lane >= components * n) & (lane < components * (n + 1))
            side = (lane >= rows) & (lane < rows + cols) & (((lane - rows) & (LANES - 1)) == n)
            mask_ref[components * n : components * (n + 1), :] = (own | side).astype(F32)

    mask = mask_ref[...]
    in_gram = lax.broadcasted_iota(jnp.int32, (rows, depth), 1) < rows
    eye_row = lax.broadcasted_iota(jnp.int32, (depth - rows, cols), 0)
    eye_col = lax.broadcasted_iota(jnp.int32, (depth - rows, cols), 1)
    minus_eye = jnp.where(eye_row == eye_col, -1.0, 0.0)
    column = lax.broadcasted_iota(jnp.int32, (components, cols), 1)
    component = lax.broadcasted_iota(jnp.int32, (components, cols), 0)
    level = lax.broadcasted_iota(jnp.int32, (components, footprint * pixels), 0)
    seds = []
    for u in range(units):
        first = (step * units + u) * LANES
        counts = [count_ref[first + n] for n in range(LANES)]
        start = sed_ref[u].astype(F32)
        seds.append(
            jnp.concatenate(
                [
                    jnp.where(((column & (LANES - 1)) == n) & (component < counts[n]), start, 0.0)
                    for n in range(LANES)
                ],
                axis=0,
            )
        )
        morph = jnp.concatenate(
            [
                jnp.where(
                    level < counts[n],
                    jnp.concatenate(
                        [morph_ref[u * LANES + n, f].astype(F32) for f in range(footprint)], axis=1
                    ),
                    0.0,
                )
                for n in range(LANES)
            ],
            axis=0,
        )
        x_ref[u, 0:rows, :] = morph.astype(BF16)
        data = jnp.concatenate(
            [
                jnp.concatenate(
                    [
                        data_ref[b, pl.ds(pl.multiple_of(f * blends + first, LANES), LANES), :]
                        for f in range(footprint)
                    ],
                    axis=1,
                )
                for b in range(bands)
            ]
            + [jnp.zeros((depth - rows - cols, footprint * pixels), F32)],
            axis=0,
        )
        x_ref[u, rows:depth, :] = data.astype(BF16)
    for sweep in range(ITERS):
        grams = [dot(x_ref[u, 0:rows, :], x_ref[u], 1, 1) * mask for u in range(units)]
        for u in range(units):
            inverse = inverse_lip(jnp.where(in_gram, grams[u] * grams[u], 0.0), components)
            right = jnp.concatenate([seds[u], minus_eye], axis=0).astype(BF16)
            high = grams[u].astype(BF16)
            low = (grams[u] - high.astype(F32)).astype(BF16)
            gradient = dot(high, right, 1, 0) + dot(low, right, 1, 0)
            seds[u] = jnp.maximum(seds[u] - gradient * inverse, 0.0).astype(BF16).astype(F32)
        for u in range(units):
            right = jnp.concatenate([seds[u], minus_eye], axis=0).astype(BF16)
            left = dot(seds[u].astype(BF16), right, 1, 1)
            inverse = inverse_lip(jnp.where(in_gram, left * left, 0.0), components)
            gradient = dot(left.astype(BF16), x_ref[u], 1, 0)
            morph = x_ref[u, 0:rows, :].astype(F32)
            morph = jnp.maximum(morph - (gradient + 0.1) * inverse, 0.0)
            x_ref[u, 0:rows, :] = morph.astype(BF16)
    for u in range(units):
        first = (step * units + u) * LANES
        model = dot(seds[u].astype(BF16), x_ref[u, 0:rows, :], 0, 0)
        for b in range(bands):
            for f in range(footprint):
                model_ref[b, pl.ds(pl.multiple_of(f * blends + first, LANES), LANES), :] = model[
                    LANES * b : LANES * (b + 1), pixels * f : pixels * (f + 1)
                ]
        sed_out_ref[u] = jnp.sum(seds[u].reshape(LANES, components, cols), axis=0).astype(BF16)

    @pl.when(step == pl.num_programs(0) - 1)
    def _():
        chosen = permutation()
        for b in range(bands):
            write_band(out_ref, b, dot(chosen, model_ref[b].astype(BF16), 1, 0))


def on_device(pixel_tiles, blend_source, blend_slot, component_count, sed_start, morph_start):
    peer_count = lax.axis_size("dev")
    blend_rows, footprint = blend_source.shape
    components, bands = sed_start.shape[1:]
    entries = blend_rows * footprint
    capacity = max(2, (entries + peer_count - 1) // peer_count)
    slots = peer_count * capacity
    tile_rows, bands, pixels = pixel_tiles.shape
    asking, placing = pl.pallas_call(
        place_kernel,
        out_shape=(
            jax.ShapeDtypeStruct((peer_count, capacity), jnp.int32),
            jax.ShapeDtypeStruct((1, entries), jnp.int32),
        ),
        compiler_params=pltpu.CompilerParams(vmem_limit_bytes=16 * 2**20),
        name="place",
    )(blend_source.T, blend_slot.T)
    wanted = lax.all_to_all(asking, "dev", split_axis=0, concat_axis=0, tiled=True)
    direct = capacity % 8 == 0
    banded = (bands, slots, pixels)
    tile_shape = (peer_count, bands, capacity, pixels) if direct else banded
    tiles = pixel_tiles.transpose(1, 0, 2)
    selector, outgoing = pl.pallas_call(
        send_kernel,
        out_shape=(
            jax.ShapeDtypeStruct((tile_rows, slots), BF16),
            jax.ShapeDtypeStruct(tile_shape, BF16),
        ),
        compiler_params=pltpu.CompilerParams(vmem_limit_bytes=16 * 2**20),
        name="send",
    )(wanted, tiles)

    def exchange(wire):
        if not direct:
            wire = wire.reshape(bands, peer_count, capacity, pixels).transpose(1, 2, 0, 3)
        moved = lax.all_to_all(wire, "dev", split_axis=0, concat_axis=0, tiled=True)
        return moved if direct else moved.transpose(2, 0, 1, 3).reshape(banded)

    arrived = exchange(outgoing)
    groups = blend_rows // LANES
    units = math.gcd(groups, 4)
    rows, cols = LANES * components, LANES * bands
    depth = -(-(rows + cols) // 128) * 128
    sed_in = (
        sed_start.reshape(groups, LANES, components, bands)
        .transpose(0, 2, 3, 1)
        .reshape(groups, components, cols)
    )
    sed_blocks, models = pl.pallas_call(
        functools.partial(fit_kernel, units=units),
        grid=(groups // units,),
        in_specs=[
            pl.BlockSpec(memory_space=pltpu.SMEM),
            pl.BlockSpec(memory_space=pltpu.VMEM),
            pl.BlockSpec(memory_space=pltpu.VMEM),
            pl.BlockSpec((units, components, cols), lambda i: (i, 0, 0)),
            pl.BlockSpec((units * LANES, footprint, components, pixels), lambda i: (i, 0, 0, 0)),
        ],
        out_specs=[
            pl.BlockSpec((units, components, cols), lambda i: (i, 0, 0)),
            pl.BlockSpec(tile_shape, lambda i: (0,) * len(tile_shape)),
        ],
        out_shape=(
            jax.ShapeDtypeStruct((groups, components, cols), BF16),
            jax.ShapeDtypeStruct(tile_shape, BF16),
        ),
        scratch_shapes=[
            pltpu.VMEM((units, depth, footprint * pixels), BF16),
            pltpu.VMEM((rows, depth), F32),
            pltpu.VMEM((bands, entries, pixels), F32),
            pltpu.VMEM((bands, entries, pixels), F32),
        ],
        compiler_params=pltpu.CompilerParams(
            dimension_semantics=("arbitrary",), vmem_limit_bytes=24 * 2**20
        ),
        name="fit",
    )(component_count, placing, arrived, sed_in, morph_start)
    sed_final = (
        sed_blocks.reshape(groups, components, bands, LANES)
        .transpose(0, 3, 1, 2)
        .reshape(sed_start.shape)
    )
    returned = exchange(models)
    everyone = lax.axis_size("grp") * peer_count
    residual, partial = pl.pallas_call(
        residual_kernel,
        out_shape=(
            jax.ShapeDtypeStruct((bands, tile_rows, pixels), F32),
            jax.ShapeDtypeStruct((everyone, 1, 128), F32),
        ),
        in_specs=[pl.BlockSpec(memory_space=pltpu.VMEM)] * 3,
        out_specs=[pl.BlockSpec(memory_space=pltpu.VMEM)] * 2,
        compiler_params=pltpu.CompilerParams(vmem_limit_bytes=16 * 2**20),
        name="residual",
    )(selector, tiles, returned)
    partials = lax.all_to_all(partial, ("grp", "dev"), split_axis=0, concat_axis=0, tiled=True)
    total_sq = jnp.sum(partials[:, 0, 0])
    pixel_count = float(residual.size * everyone)
    whitened = residual / jnp.sqrt(total_sq / pixel_count + 1e-06)
    return (whitened.transpose(1, 0, 2), sed_final)


def solution(mesh):
    placed = (
        P(("grp", "dev"), None, None),
        P(("grp", "dev"), None),
        P(("grp", "dev"), None),
        P(("grp", "dev")),
        P(("grp", "dev"), None, None),
        P(("grp", "dev"), None, None, None),
    )
    return jax.shard_map(
        on_device,
        mesh=mesh,
        in_specs=placed,
        out_specs=(P(("grp", "dev"), None, None), P(("grp", "dev"), None, None)),
        check_vma=False,
    )
```
